1024 devices in a mesh: gx: 4 (over y_hi), gy: 16 (over y_lo, z), gz: 16 (over x, core).
Axes of the slice: x: 8, y: 8 (y_hi: 4, y_lo: 2; y = y_hi * 2 + y_lo), z: 8, core: 2. Of those that a mesh axis runs over, the one named last changes fastest.
Arguments:
- conserved: float32 [5, 32, 128, 2048], P(None, 'gx', 'gy', 'gz'), may hold values from -3 to 4, as said below
- sigma_guess: float32 [32, 128, 2048], P('gx', 'gy', 'gz'), may hold values from -30 to 30
Outputs:
- advanced: float32 [5, 32, 128, 2048], P(None, 'gx', 'gy', 'gz')
- sigma_field: float32 [32, 128, 2048], P('gx', 'gy', 'gz')
The draws below stay inside these ranges and needn't reach their ends.
Inputs may be any that keep to these rules, and one draw needn't show every extreme that they name: `conserved`: component 0 (density) lies between 0.5 and 2, components 1 to 3 (momenta) between -3 and 3, component 4 (energy) between 1 and 4.
All inputs are finite; a program needn't handle non-finite values.
Results may differ from the reference program's by a relative error of at most 0.00002.
Values sent between devices are 32-bit elements; how exact they have to be, the bound alone decides.
A program may use at most 64 MiB of HBM per device.

```python
import jax
import jax.numpy as jnp

SWEEPS = 4
NX = 32
NY = 128
NZ = 2048


def draw_conserved(key, part):
    key_rho = jax.random.fold_in(key, 11)
    key_mom = jax.random.fold_in(key, 12)
    key_energy = jax.random.fold_in(key, 13)
    grid_shape = (NX, NY, NZ)
    density = jax.random.uniform(key_rho, grid_shape, jnp.float32, 0.5, 2.0)
    momentum = jnp.clip(0.6 * jax.random.normal(key_mom, (3,) + grid_shape, jnp.float32), -3.0, 3.0)
    energy = jax.random.uniform(key_energy, grid_shape, jnp.float32, 1.0, 2.5)
    return jnp.concatenate([density[None], momentum, energy[None]], axis=0)


def draw_sigma_guess(key, part):
    key_sign = jax.random.fold_in(key, 21)
    key_size = jax.random.fold_in(key, 22)
    grid_shape = (NX, NY, NZ)
    sign_part = (2 * jax.random.randint(key_sign, grid_shape, 0, 2) - 1).astype(jnp.float32)
    magnitude = jax.random.uniform(key_size, grid_shape, jnp.float32, 24.0, 30.0)
    return sign_part * magnitude


def setup_inputs(seed: int = 0) -> dict:
    key_of = jax.random.split(jax.random.key(seed), 3)
    conserved = draw_conserved(jax.random.fold_in(key_of[2], 71), 0)
    sigma_guess = draw_sigma_guess(jax.random.fold_in(key_of[2], 71), 0)
    return dict(conserved=conserved, sigma_guess=sigma_guess)


ALPHA = 10.0
GAMMA = 1.4
LAMBDA = 3.0
STEP_DT = 0.4


def central(field, direction):
    return 0.5 * (jnp.roll(field, -1, direction) - jnp.roll(field, 1, direction))


def source_term(velocity):
    gradient = [[central(velocity[member], across) for across in range(3)] for member in range(3)]
    trace_sq = jnp.zeros_like(velocity[0])
    for member in range(3):
        for across in range(3):
            trace_sq = trace_sq + gradient[member][across] * gradient[across][member]
    divergence = gradient[0][0] + gradient[1][1] + gradient[2][2]
    return trace_sq + divergence * divergence


def jacobi_sweep(sigma_now, inv_density, source):
    acc_num = jnp.zeros_like(sigma_now)
    acc_den = jnp.zeros_like(sigma_now)
    for direction in range(3):
        for offset in (1, -1):
            weight_face = 0.5 * (inv_density + jnp.roll(inv_density, offset, direction))
            acc_num = acc_num + weight_face * jnp.roll(sigma_now, offset, direction)
            acc_den = acc_den + weight_face
    return (ALPHA * source + ALPHA * acc_num) / (inv_density + ALPHA * acc_den)


def physical(states, sigma_face, direction):
    density = states[0]
    normal_speed = states[1 + direction] / density
    kinetic = 0.5 * (states[1] * states[1] + states[2] * states[2] + states[3] * states[3]) / density
    pressure = (GAMMA - 1.0) * (states[4] - kinetic) + sigma_face
    flux_rows = [states[1 + direction]]
    for member in range(3):
        flux_term = states[1 + member] * normal_speed
        if member == direction:
            flux_term = flux_term + pressure
        flux_rows.append(flux_term)
    flux_rows.append((states[4] + pressure) * normal_speed)
    return jnp.stack(flux_rows)


def flux_change(conserved, sigma_field, direction):
    axis_q = direction + 1
    left_state = (5.0 * conserved + 2.0 * jnp.roll(conserved, -1, axis_q) - jnp.roll(conserved, 1, axis_q)) / 6.0
    right_state = (2.0 * conserved + 5.0 * jnp.roll(conserved, -1, axis_q) - jnp.roll(conserved, -2, axis_q)) / 6.0
    left_sigma = (5.0 * sigma_field + 2.0 * jnp.roll(sigma_field, -1, direction) - jnp.roll(sigma_field, 1, direction)) / 6.0
    right_sigma = (2.0 * sigma_field + 5.0 * jnp.roll(sigma_field, -1, direction) - jnp.roll(sigma_field, -2, direction)) / 6.0
    face_flux = 0.5 * (physical(left_state, left_sigma, direction) + physical(right_state, right_sigma, direction)) - 0.5 * LAMBDA * (right_state - left_state)
    return face_flux - jnp.roll(face_flux, 1, axis_q)


def reference(conserved, sigma_guess):
    inv_density = 1.0 / conserved[0]
    velocity = conserved[1:4] / conserved[0]
    source = source_term(velocity)
    sigma_now = sigma_guess
    for sweep_no in range(SWEEPS):
        sigma_now = jacobi_sweep(sigma_now, inv_density, source)
    tendency = jnp.zeros_like(conserved)
    for direction in range(3):
        tendency = tendency - flux_change(conserved, sigma_now, direction)
    advanced = conserved + STEP_DT * tendency
    return advanced, sigma_now
```

```python
import functools

import jax
import jax.numpy as jnp
from jax import lax
from jax.experimental import pallas as pl
from jax.experimental.pallas import tpu as pltpu
from jax.sharding import PartitionSpec as P

MESH = pl.DeviceIdType.MESH
SWEEPS = 4
ALPHA = 10.0
GAMMA = 1.4
LAMBDA = 3.0
STEP_DT = 0.4

PX, PY = 2, 8
ROWS = pl.ds(PY, 8)
PLANES = pl.ds(PX, 8)


def face_state(z, a, b, c, d):
    left = [(5.0 / 6.0) * a[k] + (1.0 / 3.0) * b[k] - (1.0 / 6.0) * z[k] for k in range(5)]
    right = [(1.0 / 3.0) * a[k] + (5.0 / 6.0) * b[k] - (1.0 / 6.0) * c[k] for k in range(5)]
    rows = [None] * 5
    speeds = []
    for side, s in enumerate((left, right)):
        inv = 1.0 / s[0]
        speed = s[1 + d] * inv
        speeds.append(speed)
        kinetic = 0.5 * (s[1] * s[1] + s[2] * s[2] + s[3] * s[3]) * inv
        pressure = (GAMMA - 1.0) * (s[4] - kinetic)
        sign = 0.5 * LAMBDA if side == 0 else -0.5 * LAMBDA
        terms = [s[1 + d]]
        for k in range(3):
            t = s[1 + k] * speed
            terms.append(t + pressure if k == d else t)
        terms.append((s[4] + pressure) * speed)
        for k in range(5):
            t = 0.5 * terms[k] + sign * s[k]
            rows[k] = t if rows[k] is None else rows[k] + t
    return rows, speeds


def kernel(sizes, q_hbm, g_hbm, adv, sig, pq, zq, sg, zs, wt, src, base, spd, lsem, ssem, rsem):
    def peer(axis, step):
        n = sizes[axis]
        return {axis: lax.rem(lax.axis_index(axis) + (step + n), n)}

    faces = [("gy", 1), ("gy", -1), ("gx", 1), ("gx", -1), ("gz", 1), ("gz", -1)]
    load_q = pltpu.make_async_copy(q_hbm, pq.at[:, PLANES, ROWS, :], lsem.at[0])
    load_g = pltpu.make_async_copy(g_hbm, sg.at[0, PLANES, ROWS, :], lsem.at[1])
    load_q.start()
    load_g.start()
    barrier = pltpu.get_barrier_semaphore()
    for axis, step in faces:
        pl.semaphore_signal(barrier, inc=1, device_id=peer(axis, step), device_id_type=MESH)
    pl.semaphore_wait(barrier, 6)
    load_q.wait()
    load_g.wait()

    used = [0]
    pending = []

    def send(source, target, axis, step):
        n = used[0]
        used[0] += 1
        copy = pltpu.make_async_remote_copy(
            src_ref=source,
            dst_ref=target,
            send_sem=ssem.at[n],
            recv_sem=rsem.at[n],
            device_id=peer(axis, step),
            device_id_type=MESH,
        )
        copy.start()
        pending.append(copy)
        return copy

    def rim_copies(ref, near, far):
        w = far - near
        lead = (slice(None),) * (len(ref.shape) - 3)

        def part(planes, rows):
            return ref.at[lead + (planes, rows, slice(None))]

        out = []
        out.append(send(part(PLANES, pl.ds(PY + 8 - far, w)), part(PLANES, pl.ds(PY - far, w)), "gy", 1))
        out.append(send(part(PLANES, pl.ds(PY + near, w)), part(PLANES, pl.ds(PY + 8 + near, w)), "gy", -1))
        out.append(send(part(pl.ds(PX + 8 - far, w), ROWS), part(pl.ds(PX - far, w), ROWS), "gx", 1))
        out.append(send(part(pl.ds(PX + near, w), ROWS), part(pl.ds(PX + 8 + near, w), ROWS), "gx", -1))
        return out

    def lane_copies(source, lower, upper):
        return [send(source, lower, "gz", 1), send(source, upper, "gz", -1)]

    first = rim_copies(pq.at[pl.ds(0, 4)], 0, 1)
    first += rim_copies(sg.at[0], 0, 1)
    first += lane_copies(pq.at[pl.ds(0, 4), PLANES, ROWS, :], zq.at[0, pl.ds(0, 4)], zq.at[1, pl.ds(0, 4)])
    first += lane_copies(sg.at[0, PLANES, ROWS, :], zs.at[0, 0], zs.at[0, 1])
    second = rim_copies(pq.at[pl.ds(0, 4)], 1, 2)
    second += rim_copies(pq.at[pl.ds(4, 1)], 0, 2)
    second += lane_copies(pq.at[4, PLANES, ROWS, :], zq.at[0, 4], zq.at[1, 4])

    lane = lax.broadcasted_iota(jnp.int32, (8, 128), 1)

    def from_below(x, lower, n):
        return pltpu.roll(jnp.where(lane >= 128 - n, lower, x), n, 1)

    def from_above(x, upper, n):
        return pltpu.roll(jnp.where(lane < n, upper, x), 128 - n, 1)

    for copy in first:
        copy.wait_recv()

    def prepare(i):
        x = i + PX

        def primitive(plane, row):
            inv = 1.0 / pq[0, plane, pl.ds(row, 8), :]
            return [inv] + [pq[1 + k, plane, pl.ds(row, 8), :] * inv for k in range(3)]

        centre = primitive(x, PY)
        lo_inv = 1.0 / zq[0, 0, i]
        hi_inv = 1.0 / zq[1, 0, i]
        lo = [lo_inv] + [zq[0, 1 + k, i] * lo_inv for k in range(3)]
        hi = [hi_inv] + [zq[1, 1 + k, i] * hi_inv for k in range(3)]
        pairs = [
            (primitive(x - 1, PY), primitive(x + 1, PY)),
            (primitive(x, PY - 1), primitive(x, PY + 1)),
            ([from_below(centre[k], lo[k], 1) for k in range(4)], [from_above(centre[k], hi[k], 1) for k in range(4)]),
        ]
        grad = [[0.5 * (pairs[j][1][1 + k] - pairs[j][0][1 + k]) for j in range(3)] for k in range(3)]
        div = grad[0][0] + grad[1][1] + grad[2][2]
        source = div * div
        for k in range(3):
            source = source + grad[k][k] * grad[k][k]
        source = source + 2.0 * (grad[0][1] * grad[1][0] + grad[0][2] * grad[2][0] + grad[1][2] * grad[2][1])
        weights = [0.5 * (centre[0] + pairs[j][e][0]) for j in range(3) for e in range(2)]
        total = weights[0]
        for w in weights[1:]:
            total = total + w
        scale = ALPHA / (centre[0] + ALPHA * total)
        src[i] = source * scale
        for n in range(6):
            wt[n, i] = weights[n] * scale

    for i in range(8):
        prepare(i)

    def sweep(s):
        for i in range(8):
            x = i + PX
            here = sg[s, x, ROWS, :]
            near = [
                sg[s, x - 1, ROWS, :],
                sg[s, x + 1, ROWS, :],
                sg[s, x, pl.ds(PY - 1, 8), :],
                sg[s, x, pl.ds(PY + 1, 8), :],
                from_below(here, zs[s, 0, i], 1),
                from_above(here, zs[s, 1, i], 1),
            ]
            value = src[i]
            for n in range(6):
                value = value + wt[n, i] * near[n]
            sg[s + 1, x, ROWS, :] = value

    def sigma_copies(s, width):
        copies = rim_copies(sg.at[s], 0, width)
        return copies + lane_copies(sg.at[s, PLANES, ROWS, :], zs.at[s, 0], zs.at[s, 1])

    def stencil(fields, i, d):
        x = i + PX
        if d == 0:
            return [[pq[k, x + o, ROWS, :] for k in fields] for o in range(-2, 3)]
        if d == 1:
            return [[pq[k, x, pl.ds(PY + o, 8), :] for k in fields] for o in range(-2, 3)]
        here = [pq[k, x, ROWS, :] for k in fields]
        lo = [zq[0, k, i] for k in fields]
        hi = [zq[1, k, i] for k in fields]
        out = []
        for o in (2, 1):
            out.append([from_below(here[k], lo[k], o) for k in fields])
        out.append(here)
        for o in (1, 2):
            out.append([from_above(here[k], hi[k], o) for k in fields])
        return out

    def base_flux(d):
        def body(i, carry):
            q = stencil(range(5), i, d)
            low, low_speed = face_state(q[0], q[1], q[2], q[3], d)
            high, high_speed = face_state(q[1], q[2], q[3], q[4], d)
            for k in range(5):
                start = pq[k, i + PX, ROWS, :] if d == 0 else base[k, i]
                base[k, i] = start - STEP_DT * (high[k] - low[k])
            for n, v in enumerate(low_speed + high_speed):
                spd[4 * d + n, i] = v * (0.5 * STEP_DT)
            return carry

        lax.fori_loop(0, 8, body, 0)

    rounds = None
    for s in range(SWEEPS):
        if s:
            for copy in rounds:
                copy.wait_recv()
        sweep(s)
        rounds = sigma_copies(s + 1, 1 if s + 1 < SWEEPS else 2)
        if s == 0:
            for copy in second:
                copy.wait_recv()
        if s < 3:
            base_flux(s)
        else:
            for i in range(8):
                sig[i] = sg[SWEEPS, i + PX, ROWS, :]
    for copy in rounds:
        copy.wait_recv()

    for i in range(8):
        x = i + PX
        here = sg[SWEEPS, x, ROWS, :]
        lo, hi = zs[SWEEPS, 0, i], zs[SWEEPS, 1, i]
        lines = [
            [sg[SWEEPS, x + o, ROWS, :] for o in range(-2, 3)],
            [sg[SWEEPS, x, pl.ds(PY + o, 8), :] for o in range(-2, 3)],
            [from_below(here, lo, 2), from_below(here, lo, 1), here, from_above(here, hi, 1), from_above(here, hi, 2)],
        ]
        adv[0, i] = base[0, i]
        energy = base[4, i]
        for d in range(3):
            v = lines[d]
            left = [(5.0 / 6.0) * v[1 + e] + (1.0 / 3.0) * v[2 + e] - (1.0 / 6.0) * v[e] for e in range(2)]
            right = [(1.0 / 3.0) * v[1 + e] + (5.0 / 6.0) * v[2 + e] - (1.0 / 6.0) * v[3 + e] for e in range(2)]
            adv[1 + d, i] = base[1 + d, i] - (0.5 * STEP_DT) * ((left[1] + right[1]) - (left[0] + right[0]))
            energy = energy - (
                (left[1] * spd[4 * d + 2, i] + right[1] * spd[4 * d + 3, i])
                - (left[0] * spd[4 * d, i] + right[0] * spd[4 * d + 1, i])
            )
        adv[4, i] = energy

    for copy in pending:
        copy.wait_send()


N_COPIES = 12 + 10 + 6 * SWEEPS


def solution(mesh):
    sizes = {a: mesh.shape[a] for a in ("gx", "gy", "gz")}

    def on_device(conserved, sigma_guess):
        f32 = jnp.float32
        anywhere = pl.BlockSpec(memory_space=pl.ANY)
        vmem = pl.BlockSpec(memory_space=pltpu.VMEM)
        return pl.pallas_call(
            functools.partial(kernel, sizes),
            out_shape=(
                jax.ShapeDtypeStruct((5, 8, 8, 128), f32),
                jax.ShapeDtypeStruct((8, 8, 128), f32),
            ),
            in_specs=[anywhere, anywhere],
            out_specs=(vmem, vmem),
            scratch_shapes=[
                pltpu.VMEM((5, 12, 24, 128), f32),
                pltpu.VMEM((2, 5, 8, 8, 128), f32),
                pltpu.VMEM((SWEEPS + 1, 12, 24, 128), f32),
                pltpu.VMEM((SWEEPS + 1, 2, 8, 8, 128), f32),
                pltpu.VMEM((6, 8, 8, 128), f32),
                pltpu.VMEM((8, 8, 128), f32),
                pltpu.VMEM((5, 8, 8, 128), f32),
                pltpu.VMEM((12, 8, 8, 128), f32),
                pltpu.SemaphoreType.DMA((2,)),
                pltpu.SemaphoreType.DMA((N_COPIES,)),
                pltpu.SemaphoreType.DMA((N_COPIES,)),
            ],
            compiler_params=pltpu.CompilerParams(collective_id=0, has_side_effects=True),
        )(conserved, sigma_guess)

    return jax.shard_map(
        on_device,
        mesh=mesh,
        in_specs=(P(None, "gx", "gy", "gz"), P("gx", "gy", "gz")),
        out_specs=(P(None, "gx", "gy", "gz"), P("gx", "gy", "gz")),
        check_vma=False,
    )
```

```python
import functools

import jax
import jax.numpy as jnp
from jax import lax
from jax.experimental import pallas as pl
from jax.experimental.pallas import tpu as pltpu
from jax.sharding import PartitionSpec as P

MESH = pl.DeviceIdType.MESH
SWEEPS = 4
ALPHA = 10.0
GAMMA = 1.4
LAMBDA = 3.0
STEP_DT = 0.4

PX, PY = 3, 8
N_X, N_Y = 14, 24
ROWS = pl.ds(PY, 8)
PLANES = pl.ds(PX, 8)
FACES = [(0, 1, 0), (0, -1, 0), (1, 0, 0), (-1, 0, 0), (0, 0, 1), (0, 0, -1)]
EDGES = [(i, j, k) for i in (1, -1, 0) for j in (1, -1, 0) for k in (1, -1, 0) if abs(i) + abs(j) + abs(k) == 2]


def face_state(z, a, b, c, d):
    left = [(5.0 / 6.0) * a[k] + (1.0 / 3.0) * b[k] - (1.0 / 6.0) * z[k] for k in range(5)]
    right = [(1.0 / 3.0) * a[k] + (5.0 / 6.0) * b[k] - (1.0 / 6.0) * c[k] for k in range(5)]
    rows = [None] * 5
    speeds = []
    for side, s in enumerate((left, right)):
        inv = 1.0 / s[0]
        speed = s[1 + d] * inv
        speeds.append(speed)
        kinetic = 0.5 * (s[1] * s[1] + s[2] * s[2] + s[3] * s[3]) * inv
        pressure = (GAMMA - 1.0) * (s[4] - kinetic)
        sign = 0.5 * LAMBDA if side == 0 else -0.5 * LAMBDA
        terms = [s[1 + d]]
        for k in range(3):
            t = s[1 + k] * speed
            terms.append(t + pressure if k == d else t)
        terms.append((s[4] + pressure) * speed)
        for k in range(5):
            t = 0.5 * terms[k] + sign * s[k]
            rows[k] = t if rows[k] is None else rows[k] + t
    return rows, speeds


def kernel(
    sizes, q_hbm, g_hbm, adv, sig, pq, zq, sg, zs, src, zsrc, wt, sw, wb, sb, base, spd, lsem, ssem, rsem
):
    def peer(offset):
        out = {}
        for axis, step in zip(("gx", "gy", "gz"), offset):
            if step:
                n = sizes[axis]
                out[axis] = lax.rem(lax.axis_index(axis) + (step + n), n)
        return out

    load_q = pltpu.make_async_copy(q_hbm, pq.at[:, PLANES, ROWS, :], lsem.at[0])
    load_g = pltpu.make_async_copy(g_hbm, sg.at[0, PLANES, ROWS, :], lsem.at[1])
    load_q.start()
    load_g.start()
    barrier = pltpu.get_barrier_semaphore()
    for offset in FACES:
        pl.semaphore_signal(barrier, inc=1, device_id=peer(offset), device_id_type=MESH)
    pl.semaphore_wait(barrier, 6)
    load_q.wait()
    load_g.wait()

    pending = []

    def send(source, target, offset):
        n = len(pending)
        copy = pltpu.make_async_remote_copy(
            src_ref=source,
            dst_ref=target,
            send_sem=ssem.at[n],
            recv_sem=rsem.at[n],
            device_id=peer(offset),
            device_id_type=MESH,
        )
        copy.start()
        pending.append(copy)
        return copy

    def span(step, start, near, far):
        w = far - near
        if step == 0:
            return pl.ds(start, 8), pl.ds(start, 8)
        if step > 0:
            return pl.ds(start + 8 - far, w), pl.ds(start - far, w)
        return pl.ds(start + near, w), pl.ds(start + 8 + near, w)

    def share(offset, centre, lower, upper, near, far, near_y=None, far_y=None):
        planes, planes_to = span(offset[0], PX, near, far)
        rows, rows_to = span(offset[1], PY, near if near_y is None else near_y, far if far_y is None else far_y)
        lead = (slice(None),) * (len(centre.shape) - 3)
        target = {0: centre, 1: lower, -1: upper}[offset[2]]
        return send(
            centre.at[lead + (planes, rows, slice(None))],
            target.at[lead + (planes_to, rows_to, slice(None))],
            offset,
        )

    def sigma(s):
        return sg.at[s], zs.at[s, 0], zs.at[s, 1]

    def fields(a, n):
        k = pl.ds(a, n)
        return pq.at[k], zq.at[0, k], zq.at[1, k]

    first = [share(o, *fields(0, 4), 0, 1) for o in FACES]
    first += [share(o, *sigma(0), 0, 1) for o in FACES]
    second = [share(o, *fields(0, 4), 1, 2) for o in FACES[:4]]
    second += [share(o, *fields(4, 1), 0, 2) for o in FACES]

    lane = lax.broadcasted_iota(jnp.int32, (8, 128), 1)

    def from_below(x, lower, n):
        return pltpu.roll(jnp.where(lane >= 128 - n, lower, x), n, 1)

    def from_above(x, upper, n):
        return pltpu.roll(jnp.where(lane < n, upper, x), 128 - n, 1)

    def strip(lower, here, upper):
        outer = jnp.where(lane >= 64, lower, here)
        inner = jnp.where(lane >= 64, here, upper)
        return jnp.where((lane >= 32) & (lane < 96), pltpu.roll(inner, 64, 1), outer)

    for copy in first:
        copy.wait_recv()
    corner = [share(o, *fields(0, 1), 0, 1) for o in EDGES]

    def scaled(centre, around):
        weights = [0.5 * (centre + n) for n in around]
        total = weights[0]
        for w in weights[1:]:
            total = total + w
        scale = ALPHA / (centre + ALPHA * total)
        return scale, [w * scale for w in weights]

    def prepare(i):
        x = i + PX

        def primitive(plane, row):
            inv = 1.0 / pq[0, plane, pl.ds(row, 8), :]
            return [inv] + [pq[1 + k, plane, pl.ds(row, 8), :] * inv for k in range(3)]

        def beyond(side):
            inv = 1.0 / zq[side, 0, x, ROWS, :]
            return [inv] + [zq[side, 1 + k, x, ROWS, :] * inv for k in range(3)]

        centre = primitive(x, PY)
        lo, hi = beyond(0), beyond(1)
        pairs = [
            (primitive(x - 1, PY), primitive(x + 1, PY)),
            (primitive(x, PY - 1), primitive(x, PY + 1)),
            ([from_below(centre[k], lo[k], 1) for k in range(4)], [from_above(centre[k], hi[k], 1) for k in range(4)]),
        ]
        grad = [[0.5 * (pairs[j][1][1 + k] - pairs[j][0][1 + k]) for j in range(3)] for k in range(3)]
        div = grad[0][0] + grad[1][1] + grad[2][2]
        source = div * div
        for k in range(3):
            source = source + grad[k][k] * grad[k][k]
        source = source + 2.0 * (grad[0][1] * grad[1][0] + grad[0][2] * grad[2][0] + grad[1][2] * grad[2][1])
        scale, weights = scaled(centre[0], [pairs[j][e][0] for j in range(3) for e in range(2)])
        src[x, ROWS, :] = source
        sw[x, ROWS, :] = source * scale
        for n in range(6):
            wt[n, x, ROWS, :] = weights[n]

    for i in range(8):
        prepare(i)
    sources = (src, zsrc.at[0], zsrc.at[1])
    outer = [share(o, *sources, 0, 1) for o in FACES]

    def relax(s, x, row):
        r = pl.ds(row, 8)
        here = sg[s, x, r, :]
        near = [
            sg[s, x - 1, r, :],
            sg[s, x + 1, r, :],
            sg[s, x, pl.ds(row - 1, 8), :],
            sg[s, x, pl.ds(row + 1, 8), :],
            from_below(here, zs[s, 0, x, r, :], 1),
            from_above(here, zs[s, 1, x, r, :], 1),
        ]
        value = sw[x, r, :]
        for n in range(6):
            value = value + wt[n, x, r, :] * near[n]
        sg[s + 1, x, r, :] = value

    def strip_of(centre, lower, upper):
        return lambda x, row: strip(*[v[x, pl.ds(row, 8), :] for v in (lower, centre, upper)])

    def relax_strips(s):
        at = strip_of(*sigma(s))
        level = [at(x, PY) for x in range(PX - 1, PX + 9)]
        for i in range(8):
            x = i + PX
            here = level[i + 1]
            near = [
                level[i],
                level[i + 2],
                at(x, PY - 1),
                at(x, PY + 1),
                pltpu.roll(here, 1, 1),
                pltpu.roll(here, 127, 1),
            ]
            value = sb[i]
            for n in range(6):
                value = value + wb[n, i] * near[n]
            zs[s + 1, 0, x, ROWS, :] = value
            zs[s + 1, 1, x, ROWS, :] = pltpu.roll(value, 64, 1)

    def relax_wide(s, depth):
        for x in [*range(PX - depth, PX), *range(PX + 8, PX + 8 + depth)]:
            relax(s, x, PY)
        for x in range(PX, PX + 8):
            relax(s, x, PY - depth)
            relax(s, x, PY + depth)
        relax_strips(s)

    def widen_tile(x, row):
        r = pl.ds(row, 8)
        centre = 1.0 / pq[0, x, r, :]
        scale, weights = scaled(
            centre,
            [
                1.0 / pq[0, x - 1, r, :],
                1.0 / pq[0, x + 1, r, :],
                1.0 / pq[0, x, pl.ds(row - 1, 8), :],
                1.0 / pq[0, x, pl.ds(row + 1, 8), :],
                from_below(centre, 1.0 / zq[0, 0, x, r, :], 1),
                from_above(centre, 1.0 / zq[1, 0, x, r, :], 1),
            ],
        )
        sw[x, r, :] = src[x, r, :] * scale
        for n in range(6):
            wt[n, x, r, :] = weights[n]

    def widen(depth):
        for x in [*range(PX - depth, PX), *range(PX + 8, PX + 8 + depth)]:
            widen_tile(x, PY)
        density = strip_of(pq.at[0], zq.at[0, 0], zq.at[1, 0])
        source = strip_of(src, zsrc.at[0], zsrc.at[1])

        def body(i, carry):
            x = i + PX
            widen_tile(x, PY - depth)
            widen_tile(x, PY + depth)
            if depth > 1:
                return carry
            centre = 1.0 / density(x, PY)
            scale, weights = scaled(
                centre,
                [
                    1.0 / density(x - 1, PY),
                    1.0 / density(x + 1, PY),
                    1.0 / density(x, PY - 1),
                    1.0 / density(x, PY + 1),
                    pltpu.roll(centre, 1, 1),
                    pltpu.roll(centre, 127, 1),
                ],
            )
            sb[i] = source(x, PY) * scale
            for n in range(6):
                wb[n, i] = weights[n]
            return carry

        lax.fori_loop(0, 8, body, 0)

    def stencil(i, d):
        x = i + PX
        if d == 0:
            return [[pq[k, x + o, ROWS, :] for k in range(5)] for o in range(-2, 3)]
        if d == 1:
            return [[pq[k, x, pl.ds(PY + o, 8), :] for k in range(5)] for o in range(-2, 3)]
        here = [pq[k, x, ROWS, :] for k in range(5)]
        lo = [zq[0, k, x, ROWS, :] for k in range(5)]
        hi = [zq[1, k, x, ROWS, :] for k in range(5)]
        out = [[from_below(here[k], lo[k], o) for k in range(5)] for o in (2, 1)]
        out.append(here)
        out += [[from_above(here[k], hi[k], o) for k in range(5)] for o in (1, 2)]
        return out

    def base_flux(d):
        def body(i, carry):
            q = stencil(i, d)
            low, low_speed = face_state(q[0], q[1], q[2], q[3], d)
            high, high_speed = face_state(q[1], q[2], q[3], q[4], d)
            for k in range(5):
                start = pq[k, i + PX, ROWS, :] if d == 0 else base[k, i]
                base[k, i] = start - STEP_DT * (high[k] - low[k])
            for n, v in enumerate(low_speed + high_speed):
                spd[4 * d + n, i] = v * (0.5 * STEP_DT)
            return carry

        lax.fori_loop(0, 8, body, 0)

    for x in range(PX, PX + 8):
        relax(0, x, PY)
    rounds = [share(o, *sigma(1), 0, 1) for o in EDGES]
    rounds += [share(o, *sigma(1), 0, 2) for o in FACES]
    late = [share(o, *sources, 1, 2) for o in FACES[:4]]
    late += [share(o, *fields(0, 1), 2, 3) for o in FACES[:4]]
    for o in EDGES:
        if o[2]:
            late.append(share(o, *fields(0, 1), 1, 2))
        else:
            late.append(share(o, *fields(0, 1), 1, 2, 0, 1))
            late.append(share(o, *fields(0, 1), 0, 1, 1, 2))

    for copy in second:
        copy.wait_recv()
    base_flux(0)
    base_flux(1)
    for copy in corner + outer:
        copy.wait_recv()
    widen(1)
    for copy in rounds:
        copy.wait_recv()
    relax_wide(1, 1)
    for x in range(PX, PX + 8):
        relax(2, x, PY)
    rounds = [share(o, *sigma(3), 0, 2) for o in EDGES] + [share(o, *sigma(3), 0, 3) for o in FACES]
    base_flux(2)
    for copy in late:
        copy.wait_recv()
    widen(2)
    for copy in rounds:
        copy.wait_recv()
    relax_wide(3, 2)

    for i in range(8):
        x = i + PX
        here = sg[SWEEPS, x, ROWS, :]
        sig[i] = here
        lo, hi = zs[SWEEPS, 0, x, ROWS, :], zs[SWEEPS, 1, x, ROWS, :]
        lines = [
            [sg[SWEEPS, x + o, ROWS, :] for o in range(-2, 3)],
            [sg[SWEEPS, x, pl.ds(PY + o, 8), :] for o in range(-2, 3)],
            [from_below(here, lo, 2), from_below(here, lo, 1), here, from_above(here, hi, 1), from_above(here, hi, 2)],
        ]
        adv[0, i] = base[0, i]
        energy = base[4, i]
        for d in range(3):
            v = lines[d]
            left = [(5.0 / 6.0) * v[1 + e] + (1.0 / 3.0) * v[2 + e] - (1.0 / 6.0) * v[e] for e in range(2)]
            right = [(1.0 / 3.0) * v[1 + e] + (5.0 / 6.0) * v[2 + e] - (1.0 / 6.0) * v[3 + e] for e in range(2)]
            adv[1 + d, i] = base[1 + d, i] - (0.5 * STEP_DT) * ((left[1] + right[1]) - (left[0] + right[0]))
            energy = energy - (
                (left[1] * spd[4 * d + 2, i] + right[1] * spd[4 * d + 3, i])
                - (left[0] * spd[4 * d, i] + right[0] * spd[4 * d + 1, i])
            )
        adv[4, i] = energy

    for copy in pending:
        copy.wait_send()


def write_out(adv, sig, adv_out, sig_out, sem):
    a = pltpu.make_async_copy(adv, adv_out, sem.at[0])
    b = pltpu.make_async_copy(sig, sig_out, sem.at[1])
    a.start()
    b.start()
    a.wait()
    b.wait()


N_COPIES = 100


def solution(mesh):
    sizes = {a: mesh.shape[a] for a in ("gx", "gy", "gz")}

    def on_device(conserved, sigma_guess):
        f32 = jnp.float32
        anywhere = pl.BlockSpec(memory_space=pl.ANY)
        vmem = pl.BlockSpec(memory_space=pltpu.VMEM)
        shapes = (
            jax.ShapeDtypeStruct((5, 8, 8, 128), f32),
            jax.ShapeDtypeStruct((8, 8, 128), f32),
        )
        made = pl.pallas_call(
            functools.partial(kernel, sizes),
            out_shape=shapes,
            in_specs=[anywhere, anywhere],
            out_specs=(vmem, vmem),
            scratch_shapes=[
                pltpu.VMEM((5, N_X, N_Y, 128), f32),
                pltpu.VMEM((2, 5, N_X, N_Y, 128), f32),
                pltpu.VMEM((SWEEPS + 1, N_X, N_Y, 128), f32),
                pltpu.VMEM((SWEEPS + 1, 2, N_X, N_Y, 128), f32),
                pltpu.VMEM((N_X, N_Y, 128), f32),
                pltpu.VMEM((2, N_X, N_Y, 128), f32),
                pltpu.VMEM((6, N_X, N_Y, 128), f32),
                pltpu.VMEM((N_X, N_Y, 128), f32),
                pltpu.VMEM((6, 8, 8, 128), f32),
                pltpu.VMEM((8, 8, 128), f32),
                pltpu.VMEM((5, 8, 8, 128), f32),
                pltpu.VMEM((12, 8, 8, 128), f32),
                pltpu.SemaphoreType.DMA((2,)),
                pltpu.SemaphoreType.DMA((N_COPIES,)),
                pltpu.SemaphoreType.DMA((N_COPIES,)),
            ],
            compiler_params=pltpu.CompilerParams(collective_id=0, has_side_effects=True, vmem_limit_bytes=16777216),
        )(*[pltpu.with_memory_space_constraint(v, pltpu.HBM) for v in (conserved, sigma_guess)])
        return pl.pallas_call(
            write_out,
            out_shape=shapes,
            in_specs=[vmem, vmem],
            out_specs=(anywhere, anywhere),
            scratch_shapes=[pltpu.SemaphoreType.DMA((2,))],
            compiler_params=pltpu.CompilerParams(vmem_limit_bytes=16777216),
        )(*made)

    return jax.shard_map(
        on_device,
        mesh=mesh,
        in_specs=(P(None, "gx", "gy", "gz"), P("gx", "gy", "gz")),
        out_specs=(P(None, "gx", "gy", "gz"), P("gx", "gy", "gz")),
        check_vma=False,
    )
```

```python
import functools

import jax
import jax.numpy as jnp
from jax import lax
from jax.experimental import pallas as pl
from jax.experimental.pallas import tpu as pltpu
from jax.sharding import PartitionSpec as P

MESH = pl.DeviceIdType.MESH
SWEEPS = 4
ALPHA = 10.0
GAMMA = 1.4
LAMBDA = 3.0
STEP_DT = 0.4

PX, PY = 3, 8
N_X, N_Y = 14, 24
ROWS = pl.ds(PY, 8)
PLANES = pl.ds(PX, 8)
FACES = [(0, 1, 0), (0, -1, 0), (1, 0, 0), (-1, 0, 0), (0, 0, 1), (0, 0, -1)]
FIRST, DENSITY, ENERGY, SOURCE, SIGMA_1, LATE, SECOND, SIGMA_3 = range(8)
N_GROUPS = 8
EDGES = [(i, j, k) for i in (1, -1, 0) for j in (1, -1, 0) for k in (1, -1, 0) if abs(i) + abs(j) + abs(k) == 2]


def face_state(z, a, b, c, d):
    left = [(5.0 / 6.0) * a[k] + (1.0 / 3.0) * b[k] - (1.0 / 6.0) * z[k] for k in range(5)]
    right = [(1.0 / 3.0) * a[k] + (5.0 / 6.0) * b[k] - (1.0 / 6.0) * c[k] for k in range(5)]
    rows = [None] * 5
    speeds = []
    for side, s in enumerate((left, right)):
        inv = 1.0 / s[0]
        speed = s[1 + d] * inv
        speeds.append(speed)
        kinetic = 0.5 * (s[1] * s[1] + s[2] * s[2] + s[3] * s[3]) * inv
        pressure = (GAMMA - 1.0) * (s[4] - kinetic)
        sign = 0.5 * LAMBDA if side == 0 else -0.5 * LAMBDA
        terms = [s[1 + d]]
        for k in range(3):
            t = s[1 + k] * speed
            terms.append(t + pressure if k == d else t)
        terms.append((s[4] + pressure) * speed)
        for k in range(5):
            t = 0.5 * terms[k] + sign * s[k]
            rows[k] = t if rows[k] is None else rows[k] + t
    return rows, speeds


def kernel(
    sizes, q_hbm, g_hbm, adv, sig, pq, zq, sg, zs, src, zsrc, wt, sw, wb, sb, base, spd, rows_ref, lsem, ssem, rsem
):
    def peer(offset):
        out = {}
        for axis, step in zip(("gx", "gy", "gz"), offset):
            if step:
                n = sizes[axis]
                out[axis] = lax.rem(lax.axis_index(axis) + (step + n), n)
        return out

    load_q = pltpu.make_async_copy(q_hbm, pq.at[:, PLANES, ROWS, :], lsem.at[0])
    load_g = pltpu.make_async_copy(g_hbm, sg.at[0, PLANES, ROWS, :], lsem.at[1])
    load_q.start()
    load_g.start()
    barrier = pltpu.get_barrier_semaphore()
    for offset in FACES:
        pl.semaphore_signal(barrier, inc=1, device_id=peer(offset), device_id_type=MESH)
    pl.semaphore_wait(barrier, 6)
    load_q.wait()
    load_g.wait()

    sent = [0] * N_GROUPS

    def send(source, target, offset, group):
        rows = 1
        for n in source.shape[:-1]:
            rows *= n
        sent[group] += rows
        pltpu.make_async_remote_copy(
            src_ref=source,
            dst_ref=target,
            send_sem=ssem.at[0],
            recv_sem=rsem.at[group],
            device_id=peer(offset),
            device_id_type=MESH,
        ).start()

    def all_rows(rows, group):
        span_ref = rows_ref.at[pl.ds(0, rows)]
        return pltpu.make_async_remote_copy(
            src_ref=span_ref,
            dst_ref=span_ref,
            send_sem=ssem.at[0],
            recv_sem=rsem.at[group],
            device_id=peer(FACES[0]),
            device_id_type=MESH,
        )

    def arrived(*groups):
        for group in groups:
            all_rows(sent[group], group).wait_recv()

    def span(step, start, near, far):
        w = far - near
        if step == 0:
            return pl.ds(start, 8), pl.ds(start, 8)
        if step > 0:
            return pl.ds(start + 8 - far, w), pl.ds(start - far, w)
        return pl.ds(start + near, w), pl.ds(start + 8 + near, w)

    def share(group, offset, centre, lower, upper, near, far, near_y=None, far_y=None):
        planes, planes_to = span(offset[0], PX, near, far)
        rows, rows_to = span(offset[1], PY, near if near_y is None else near_y, far if far_y is None else far_y)
        lead = (slice(None),) * (len(centre.shape) - 3)
        target = {0: centre, 1: lower, -1: upper}[offset[2]]
        send(
            centre.at[lead + (planes, rows, slice(None))],
            target.at[lead + (planes_to, rows_to, slice(None))],
            offset,
            group,
        )

    def sigma(s):
        return sg.at[s], zs.at[s, 0], zs.at[s, 1]

    def fields(a, n):
        k = pl.ds(a, n)
        return pq.at[k], zq.at[0, k], zq.at[1, k]

    for o in FACES:
        share(FIRST, o, *fields(0, 4), 0, 1)
        share(FIRST, o, *sigma(0), 0, 1)

    lane = lax.broadcasted_iota(jnp.int32, (8, 128), 1)

    def from_below(x, lower, n):
        return pltpu.roll(jnp.where(lane >= 128 - n, lower, x), n, 1)

    def from_above(x, upper, n):
        return pltpu.roll(jnp.where(lane < n, upper, x), 128 - n, 1)

    def strip(lower, here, upper):
        outer = jnp.where(lane >= 64, lower, here)
        inner = jnp.where(lane >= 64, here, upper)
        return jnp.where((lane >= 32) & (lane < 96), pltpu.roll(inner, 64, 1), outer)

    arrived(FIRST)
    for o in EDGES:
        share(DENSITY, o, *fields(0, 1), 0, 1)
    for o in FACES[:4]:
        share(DENSITY, o, *fields(0, 1), 1, 2)
    for o in FACES[4:]:
        share(ENERGY, o, *fields(4, 1), 0, 2)

    def scaled(centre, around):
        weights = [0.5 * (centre + n) for n in around]
        total = weights[0]
        for w in weights[1:]:
            total = total + w
        scale = ALPHA / (centre + ALPHA * total)
        return scale, [w * scale for w in weights]

    def prepare(i):
        x = i + PX

        def primitive(plane, row):
            inv = 1.0 / pq[0, plane, pl.ds(row, 8), :]
            return [inv] + [pq[1 + k, plane, pl.ds(row, 8), :] * inv for k in range(3)]

        def beyond(side):
            inv = 1.0 / zq[side, 0, x, ROWS, :]
            return [inv] + [zq[side, 1 + k, x, ROWS, :] * inv for k in range(3)]

        centre = primitive(x, PY)
        lo, hi = beyond(0), beyond(1)
        pairs = [
            (primitive(x - 1, PY), primitive(x + 1, PY)),
            (primitive(x, PY - 1), primitive(x, PY + 1)),
            ([from_below(centre[k], lo[k], 1) for k in range(4)], [from_above(centre[k], hi[k], 1) for k in range(4)]),
        ]
        grad = [[0.5 * (pairs[j][1][1 + k] - pairs[j][0][1 + k]) for j in range(3)] for k in range(3)]
        div = grad[0][0] + grad[1][1] + grad[2][2]
        source = div * div
        for k in range(3):
            source = source + grad[k][k] * grad[k][k]
        source = source + 2.0 * (grad[0][1] * grad[1][0] + grad[0][2] * grad[2][0] + grad[1][2] * grad[2][1])
        scale, weights = scaled(centre[0], [pairs[j][e][0] for j in range(3) for e in range(2)])
        src[x, ROWS, :] = source
        sw[x, ROWS, :] = source * scale
        for n in range(6):
            wt[n, x, ROWS, :] = weights[n]

    def relax(s, x, row):
        r = pl.ds(row, 8)
        here = sg[s, x, r, :]
        near = [
            sg[s, x - 1, r, :],
            sg[s, x + 1, r, :],
            sg[s, x, pl.ds(row - 1, 8), :],
            sg[s, x, pl.ds(row + 1, 8), :],
            from_below(here, zs[s, 0, x, r, :], 1),
            from_above(here, zs[s, 1, x, r, :], 1),
        ]
        value = sw[x, r, :]
        for n in range(6):
            value = value + wt[n, x, r, :] * near[n]
        sg[s + 1, x, r, :] = value

    def strip_of(centre, lower, upper):
        return lambda x, row: strip(*[v[x, pl.ds(row, 8), :] for v in (lower, centre, upper)])

    def relax_strips(s):
        at = strip_of(*sigma(s))
        level = [at(x, PY) for x in range(PX - 1, PX + 9)]
        for i in range(8):
            x = i + PX
            here = level[i + 1]
            near = [
                level[i],
                level[i + 2],
                at(x, PY - 1),
                at(x, PY + 1),
                pltpu.roll(here, 1, 1),
                pltpu.roll(here, 127, 1),
            ]
            value = sb[i]
            for n in range(6):
                value = value + wb[n, i] * near[n]
            zs[s + 1, 0, x, ROWS, :] = value
            zs[s + 1, 1, x, ROWS, :] = pltpu.roll(value, 64, 1)

    def relax_wide(s, depth):
        for x in [*range(PX - depth, PX), *range(PX + 8, PX + 8 + depth)]:
            relax(s, x, PY)
        for x in range(PX, PX + 8):
            relax(s, x, PY - depth)
            relax(s, x, PY + depth)
        relax_strips(s)

    def widen_tile(x, row):
        r = pl.ds(row, 8)
        centre = 1.0 / pq[0, x, r, :]
        scale, weights = scaled(
            centre,
            [
                1.0 / pq[0, x - 1, r, :],
                1.0 / pq[0, x + 1, r, :],
                1.0 / pq[0, x, pl.ds(row - 1, 8), :],
                1.0 / pq[0, x, pl.ds(row + 1, 8), :],
                from_below(centre, 1.0 / zq[0, 0, x, r, :], 1),
                from_above(centre, 1.0 / zq[1, 0, x, r, :], 1),
            ],
        )
        sw[x, r, :] = src[x, r, :] * scale
        for n in range(6):
            wt[n, x, r, :] = weights[n]

    def widen(depth):
        for x in [*range(PX - depth, PX), *range(PX + 8, PX + 8 + depth)]:
            widen_tile(x, PY)
        density = strip_of(pq.at[0], zq.at[0, 0], zq.at[1, 0])
        source = strip_of(src, zsrc.at[0], zsrc.at[1])

        for i in range(8):
            x = i + PX
            widen_tile(x, PY - depth)
            widen_tile(x, PY + depth)
            if depth > 1:
                continue
            centre = 1.0 / density(x, PY)
            scale, weights = scaled(
                centre,
                [
                    1.0 / density(x - 1, PY),
                    1.0 / density(x + 1, PY),
                    1.0 / density(x, PY - 1),
                    1.0 / density(x, PY + 1),
                    pltpu.roll(centre, 1, 1),
                    pltpu.roll(centre, 127, 1),
                ],
            )
            sb[i] = source(x, PY) * scale
            for n in range(6):
                wb[n, i] = weights[n]

    def stencil(i, d):
        x = i + PX
        if d == 0:
            return [[pq[k, x + o, ROWS, :] for k in range(5)] for o in range(-2, 3)]
        if d == 1:
            return [[pq[k, x, pl.ds(PY + o, 8), :] for k in range(5)] for o in range(-2, 3)]
        here = [pq[k, x, ROWS, :] for k in range(5)]
        lo = [zq[0, k, x, ROWS, :] for k in range(5)]
        hi = [zq[1, k, x, ROWS, :] for k in range(5)]
        out = [[from_below(here[k], lo[k], o) for k in range(5)] for o in (2, 1)]
        out.append(here)
        out += [[from_above(here[k], hi[k], o) for k in range(5)] for o in (1, 2)]
        return out

    def base_flux(d):
        def body(i, carry):
            q = stencil(i, d)
            low, low_speed = face_state(q[0], q[1], q[2], q[3], d)
            high, high_speed = face_state(q[1], q[2], q[3], q[4], d)
            for k in range(5):
                start = pq[k, i + PX, ROWS, :] if d == 2 else base[k, i]
                base[k, i] = start - STEP_DT * (high[k] - low[k])
            for n, v in enumerate(low_speed + high_speed):
                spd[4 * d + n, i] = v * (0.5 * STEP_DT)
            return carry

        lax.fori_loop(0, 8, body, 0)

    sources = (src, zsrc.at[0], zsrc.at[1])
    far_edges = [o for o in EDGES if o[0]]
    near_edges = [o for o in EDGES if not o[0]]
    for planes, edges, faces in (((0, 7, 1, 6), far_edges, FACES[2:4]), ((2, 5, 3, 4), near_edges, FACES[:2] + FACES[4:])):
        for i in planes:
            prepare(i)
        for i in planes:
            relax(0, i + PX, PY)
        for o in edges:
            share(SIGMA_1, o, *sigma(1), 0, 1)
        for o in faces:
            share(SOURCE, o, *sources, 0, 1)
            share(SIGMA_1, o, *sigma(1), 0, 2)
    for o in FACES[:4]:
        share(LATE, o, *sources, 1, 2)
        share(LATE, o, *fields(0, 1), 2, 3)
    for o in EDGES:
        if o[2]:
            share(LATE, o, *fields(0, 1), 1, 2)
        else:
            share(LATE, o, *fields(0, 1), 1, 2, 0, 1)
            share(LATE, o, *fields(0, 1), 0, 1, 1, 2)
    for o in FACES[:4]:
        share(SECOND, o, *fields(1, 3), 1, 2)
        share(SECOND, o, *fields(4, 1), 0, 2)

    arrived(ENERGY)
    base_flux(2)
    arrived(DENSITY, SOURCE)
    widen(1)
    arrived(SIGMA_1)
    relax_wide(1, 1)
    for i in (0, 7, 1, 6, 2, 5):
        relax(2, i + PX, PY)
    for o in far_edges:
        share(SIGMA_3, o, *sigma(3), 0, 2)
    for o in FACES[2:4]:
        share(SIGMA_3, o, *sigma(3), 0, 3)
    for i in (3, 4):
        relax(2, i + PX, PY)
    for o in near_edges:
        share(SIGMA_3, o, *sigma(3), 0, 2)
    for o in FACES[:2] + FACES[4:]:
        share(SIGMA_3, o, *sigma(3), 0, 3)
    arrived(LATE)
    widen(2)
    arrived(SECOND)
    base_flux(0)
    base_flux(1)
    arrived(SIGMA_3)
    relax_wide(3, 2)

    for i in range(8):
        x = i + PX
        here = sg[SWEEPS, x, ROWS, :]
        sig[i] = here
        lo, hi = zs[SWEEPS, 0, x, ROWS, :], zs[SWEEPS, 1, x, ROWS, :]
        lines = [
            [sg[SWEEPS, x + o, ROWS, :] for o in range(-2, 3)],
            [sg[SWEEPS, x, pl.ds(PY + o, 8), :] for o in range(-2, 3)],
            [from_below(here, lo, 2), from_below(here, lo, 1), here, from_above(here, hi, 1), from_above(here, hi, 2)],
        ]
        adv[0, i] = base[0, i]
        total = base[4, i]
        for d in range(3):
            v = lines[d]
            left = [(5.0 / 6.0) * v[1 + e] + (1.0 / 3.0) * v[2 + e] - (1.0 / 6.0) * v[e] for e in range(2)]
            right = [(1.0 / 3.0) * v[1 + e] + (5.0 / 6.0) * v[2 + e] - (1.0 / 6.0) * v[3 + e] for e in range(2)]
            adv[1 + d, i] = base[1 + d, i] - (0.5 * STEP_DT) * ((left[1] + right[1]) - (left[0] + right[0]))
            total = total - (
                (left[1] * spd[4 * d + 2, i] + right[1] * spd[4 * d + 3, i])
                - (left[0] * spd[4 * d, i] + right[0] * spd[4 * d + 1, i])
            )
        adv[4, i] = total

    all_rows(sum(sent), FIRST).wait_send()


def write_out(adv, sig, adv_out, sig_out, sem):
    a = pltpu.make_async_copy(adv, adv_out, sem.at[0])
    b = pltpu.make_async_copy(sig, sig_out, sem.at[1])
    a.start()
    b.start()
    a.wait()
    b.wait()


def solution(mesh):
    sizes = {a: mesh.shape[a] for a in ("gx", "gy", "gz")}

    def on_device(conserved, sigma_guess):
        f32 = jnp.float32
        anywhere = pl.BlockSpec(memory_space=pl.ANY)
        vmem = pl.BlockSpec(memory_space=pltpu.VMEM)
        shapes = (
            jax.ShapeDtypeStruct((5, 8, 8, 128), f32),
            jax.ShapeDtypeStruct((8, 8, 128), f32),
        )
        made = pl.pallas_call(
            functools.partial(kernel, sizes),
            out_shape=shapes,
            in_specs=[anywhere, anywhere],
            out_specs=(vmem, vmem),
            scratch_shapes=[
                pltpu.VMEM((5, N_X, N_Y, 128), f32),
                pltpu.VMEM((2, 5, N_X, N_Y, 128), f32),
                pltpu.VMEM((SWEEPS + 1, N_X, N_Y, 128), f32),
                pltpu.VMEM((SWEEPS + 1, 2, N_X, N_Y, 128), f32),
                pltpu.VMEM((N_X, N_Y, 128), f32),
                pltpu.VMEM((2, N_X, N_Y, 128), f32),
                pltpu.VMEM((6, N_X, N_Y, 128), f32),
                pltpu.VMEM((N_X, N_Y, 128), f32),
                pltpu.VMEM((6, 8, 8, 128), f32),
                pltpu.VMEM((8, 8, 128), f32),
                pltpu.VMEM((5, 8, 8, 128), f32),
                pltpu.VMEM((12, 8, 8, 128), f32),
                pltpu.VMEM((4096, 128), f32),
                pltpu.SemaphoreType.DMA((2,)),
                pltpu.SemaphoreType.DMA((1,)),
                pltpu.SemaphoreType.DMA((N_GROUPS,)),
            ],
            compiler_params=pltpu.CompilerParams(collective_id=0, has_side_effects=True, vmem_limit_bytes=16777216),
        )(*[pltpu.with_memory_space_constraint(v, pltpu.HBM) for v in (conserved, sigma_guess)])
        return pl.pallas_call(
            write_out,
            out_shape=shapes,
            in_specs=[vmem, vmem],
            out_specs=(anywhere, anywhere),
            scratch_shapes=[pltpu.SemaphoreType.DMA((2,))],
            compiler_params=pltpu.CompilerParams(vmem_limit_bytes=16777216),
        )(*made)

    return jax.shard_map(
        on_device,
        mesh=mesh,
        in_specs=(P(None, "gx", "gy", "gz"), P("gx", "gy", "gz")),
        out_specs=(P(None, "gx", "gy", "gz"), P("gx", "gy", "gz")),
        check_vma=False,
    )
```

```python
import functools

import jax
import jax.numpy as jnp
from jax import lax
from jax.experimental import pallas as pl
from jax.experimental.pallas import tpu as pltpu
from jax.sharding import PartitionSpec as P

MESH = pl.DeviceIdType.MESH
SWEEPS = 4
ALPHA = 10.0
GAMMA = 1.4
LAMBDA = 3.0
STEP_DT = 0.4

PX, PY = 3, 8
N_X, N_Y = 14, 24
ROWS = pl.ds(PY, 8)
PLANES = pl.ds(PX, 8)
FACES = [(0, 1, 0), (0, -1, 0), (1, 0, 0), (-1, 0, 0), (0, 0, 1), (0, 0, -1)]
EDGES = [(i, j, k) for i in (1, -1, 0) for j in (1, -1, 0) for k in (1, -1, 0) if abs(i) + abs(j) + abs(k) == 2]
BESIDE = [o for o in EDGES if o[2]]
DIAGONAL = [o for o in EDGES if not o[2]]
FIRST, DENSITY, ENERGY, SOURCE, SIGMA_1, LATE, SECOND, SIGMA_3 = range(8)
N_GROUPS = 8


def face_state(z, a, b, c, d):
    left = [(5.0 / 6.0) * a[k] + (1.0 / 3.0) * b[k] - (1.0 / 6.0) * z[k] for k in range(5)]
    right = [(1.0 / 3.0) * a[k] + (5.0 / 6.0) * b[k] - (1.0 / 6.0) * c[k] for k in range(5)]
    rows = [None] * 5
    speeds = []
    for side, s in enumerate((left, right)):
        inv = 1.0 / s[0]
        speed = s[1 + d] * inv
        speeds.append(speed)
        kinetic = 0.5 * (s[1] * s[1] + s[2] * s[2] + s[3] * s[3]) * inv
        pressure = (GAMMA - 1.0) * (s[4] - kinetic)
        sign = 0.5 * LAMBDA if side == 0 else -0.5 * LAMBDA
        terms = [s[1 + d]]
        for k in range(3):
            t = s[1 + k] * speed
            terms.append(t + pressure if k == d else t)
        terms.append((s[4] + pressure) * speed)
        for k in range(5):
            t = 0.5 * terms[k] + sign * s[k]
            rows[k] = t if rows[k] is None else rows[k] + t
    return rows, speeds


def kernel(
    sizes, q_hbm, g_hbm, adv, sig, pq, zq, sg, zs, src, zsrc, wt, sw, wb, sb, base, spd, rows_ref, pk, rk, lsem, ssem, rsem
):
    def peer(offset):
        out = {}
        for axis, step in zip(("gx", "gy", "gz"), offset):
            if step:
                n = sizes[axis]
                out[axis] = lax.rem(lax.axis_index(axis) + (step + n), n)
        return out

    load_q = pltpu.make_async_copy(q_hbm, pq.at[:, PLANES, ROWS, :], lsem.at[0])
    load_g = pltpu.make_async_copy(g_hbm, sg.at[0, PLANES, ROWS, :], lsem.at[1])
    load_q.start()
    load_g.start()
    barrier = pltpu.get_barrier_semaphore()
    for offset in FACES:
        pl.semaphore_signal(barrier, inc=1, device_id=peer(offset), device_id_type=MESH)
    pl.semaphore_wait(barrier, 6)
    load_q.wait()
    load_g.wait()

    sent = [0] * N_GROUPS

    def send(source, target, offset, group):
        rows = 1
        for n in source.shape[:-1]:
            rows *= n
        sent[group] += rows
        pltpu.make_async_remote_copy(
            src_ref=source,
            dst_ref=target,
            send_sem=ssem.at[0],
            recv_sem=rsem.at[group],
            device_id=peer(offset),
            device_id_type=MESH,
        ).start()

    def all_rows(rows, group):
        span_ref = rows_ref.at[pl.ds(0, rows)]
        return pltpu.make_async_remote_copy(
            src_ref=span_ref,
            dst_ref=span_ref,
            send_sem=ssem.at[0],
            recv_sem=rsem.at[group],
            device_id=peer(FACES[0]),
            device_id_type=MESH,
        )

    def arrived(*groups):
        for group in groups:
            all_rows(sent[group], group).wait_recv()

    def span(step, start, near, far):
        w = far - near
        if step == 0:
            return pl.ds(start, 8), pl.ds(start, 8)
        if step > 0:
            return pl.ds(start + 8 - far, w), pl.ds(start - far, w)
        return pl.ds(start + near, w), pl.ds(start + 8 + near, w)

    def share(group, offset, centre, lower, upper, near, far, near_y=None, far_y=None):
        planes, planes_to = span(offset[0], PX, near, far)
        rows, rows_to = span(offset[1], PY, near if near_y is None else near_y, far if far_y is None else far_y)
        lead = (slice(None),) * (len(centre.shape) - 3)
        target = {0: centre, 1: lower, -1: upper}[offset[2]]
        send(
            centre.at[lead + (planes, rows, slice(None))],
            target.at[lead + (planes_to, rows_to, slice(None))],
            offset,
            group,
        )

    narrow = lax.broadcasted_iota(jnp.int32, (1, 128), 1)

    def place(start, step, layer, there):
        if there:
            return start - 1 - layer if step > 0 else start + 8 + layer
        return start + 7 - layer if step > 0 else start + layer

    def spot(offset, layer, i, there):
        if offset[0]:
            return place(PX, offset[0], layer, there), pl.ds(PY + i, 1)
        return PX + i, pl.ds(place(PY, offset[1], layer, there), 1)

    def turn(row, n):
        return pltpu.roll(row, n % 128, 1) if n % 128 else row

    def pack_lines(k, offsets, centre, depth):
        for offset in offsets:
            e = BESIDE.index(offset)
            for layer in range(depth):
                row = None
                for i in range(8):
                    x, r = spot(offset, layer, i, False)
                    v = turn(centre[x, r, :], 16 * i + (16 if offset[2] > 0 else 0))
                    row = v if row is None else jnp.where(narrow >= 16 * i, v, row)
                pk[k, e, pl.ds(layer, 1), :] = row

    def share_lines(group, k, offsets, depth):
        for offset in offsets:
            e = BESIDE.index(offset)
            send(pk.at[k, e, pl.ds(0, depth), :], rk.at[k, e, pl.ds(0, depth), :], offset, group)

    def spread_lines(k, lower, upper, depth):
        for e, offset in enumerate(BESIDE):
            target = lower if offset[2] > 0 else upper
            for layer in range(depth):
                row = rk[k, e, pl.ds(layer, 1), :]
                for i in range(8):
                    x, r = spot(offset, layer, i, True)
                    target[x, r, :] = turn(row, -16 * i - (16 if offset[2] > 0 else 0))

    def sigma(s):
        return sg.at[s], zs.at[s, 0], zs.at[s, 1]

    def fields(a, n):
        k = pl.ds(a, n)
        return pq.at[k], zq.at[0, k], zq.at[1, k]

    for o in FACES:
        share(FIRST, o, *fields(0, 4), 0, 1)
        share(FIRST, o, *sigma(0), 0, 1)

    lane = lax.broadcasted_iota(jnp.int32, (8, 128), 1)

    def from_below(x, lower, n):
        return pltpu.roll(jnp.where(lane >= 128 - n, lower, x), n, 1)

    def from_above(x, upper, n):
        return pltpu.roll(jnp.where(lane < n, upper, x), 128 - n, 1)

    def strip(lower, here, upper):
        outer = jnp.where(lane >= 64, lower, here)
        inner = jnp.where(lane >= 64, here, upper)
        return jnp.where((lane >= 32) & (lane < 96), pltpu.roll(inner, 64, 1), outer)

    pack_lines(0, BESIDE, pq.at[0], 2)
    arrived(FIRST)
    for o in DIAGONAL:
        share(DENSITY, o, *fields(0, 1), 0, 1)
    share_lines(DENSITY, 0, BESIDE, 2)
    for o in FACES[:4]:
        share(DENSITY, o, *fields(0, 1), 1, 2)
    for o in FACES[4:]:
        share(ENERGY, o, *fields(4, 1), 0, 2)

    def scaled(centre, around):
        weights = [0.5 * (centre + n) for n in around]
        total = weights[0]
        for w in weights[1:]:
            total = total + w
        scale = ALPHA / (centre + ALPHA * total)
        return scale, [w * scale for w in weights]

    def prepare(i):
        x = i + PX

        def primitive(plane, row):
            inv = 1.0 / pq[0, plane, pl.ds(row, 8), :]
            return [inv] + [pq[1 + k, plane, pl.ds(row, 8), :] * inv for k in range(3)]

        def beyond(side):
            inv = 1.0 / zq[side, 0, x, ROWS, :]
            return [inv] + [zq[side, 1 + k, x, ROWS, :] * inv for k in range(3)]

        centre = primitive(x, PY)
        lo, hi = beyond(0), beyond(1)
        pairs = [
            (primitive(x - 1, PY), primitive(x + 1, PY)),
            (primitive(x, PY - 1), primitive(x, PY + 1)),
            ([from_below(centre[k], lo[k], 1) for k in range(4)], [from_above(centre[k], hi[k], 1) for k in range(4)]),
        ]
        grad = [[0.5 * (pairs[j][1][1 + k] - pairs[j][0][1 + k]) for j in range(3)] for k in range(3)]
        div = grad[0][0] + grad[1][1] + grad[2][2]
        source = div * div
        for k in range(3):
            source = source + grad[k][k] * grad[k][k]
        source = source + 2.0 * (grad[0][1] * grad[1][0] + grad[0][2] * grad[2][0] + grad[1][2] * grad[2][1])
        scale, weights = scaled(centre[0], [pairs[j][e][0] for j in range(3) for e in range(2)])
        src[x, ROWS, :] = source
        sw[x, ROWS, :] = source * scale
        for n in range(6):
            wt[n, x, ROWS, :] = weights[n]

    def relax(s, x, row):
        r = pl.ds(row, 8)
        here = sg[s, x, r, :]
        near = [
            sg[s, x - 1, r, :],
            sg[s, x + 1, r, :],
            sg[s, x, pl.ds(row - 1, 8), :],
            sg[s, x, pl.ds(row + 1, 8), :],
            from_below(here, zs[s, 0, x, r, :], 1),
            from_above(here, zs[s, 1, x, r, :], 1),
        ]
        value = sw[x, r, :]
        for n in range(6):
            value = value + wt[n, x, r, :] * near[n]
        sg[s + 1, x, r, :] = value

    def strip_of(centre, lower, upper):
        return lambda x, row: strip(*[v[x, pl.ds(row, 8), :] for v in (lower, centre, upper)])

    def relax_strips(s):
        at = strip_of(*sigma(s))
        level = [at(x, PY) for x in range(PX - 1, PX + 9)]
        for i in range(8):
            x = i + PX
            here = level[i + 1]
            near = [
                level[i],
                level[i + 2],
                at(x, PY - 1),
                at(x, PY + 1),
                pltpu.roll(here, 1, 1),
                pltpu.roll(here, 127, 1),
            ]
            value = sb[i]
            for n in range(6):
                value = value + wb[n, i] * near[n]
            zs[s + 1, 0, x, ROWS, :] = value
            zs[s + 1, 1, x, ROWS, :] = pltpu.roll(value, 64, 1)

    def relax_wide(s, depth):
        for x in [*range(PX - depth, PX), *range(PX + 8, PX + 8 + depth)]:
            relax(s, x, PY)
        for x in range(PX, PX + 8):
            relax(s, x, PY - depth)
            relax(s, x, PY + depth)
        relax_strips(s)

    def widen_tile(x, row):
        r = pl.ds(row, 8)
        centre = 1.0 / pq[0, x, r, :]
        scale, weights = scaled(
            centre,
            [
                1.0 / pq[0, x - 1, r, :],
                1.0 / pq[0, x + 1, r, :],
                1.0 / pq[0, x, pl.ds(row - 1, 8), :],
                1.0 / pq[0, x, pl.ds(row + 1, 8), :],
                from_below(centre, 1.0 / zq[0, 0, x, r, :], 1),
                from_above(centre, 1.0 / zq[1, 0, x, r, :], 1),
            ],
        )
        sw[x, r, :] = src[x, r, :] * scale
        for n in range(6):
            wt[n, x, r, :] = weights[n]

    def widen(depth):
        for x in [*range(PX - depth, PX), *range(PX + 8, PX + 8 + depth)]:
            widen_tile(x, PY)
        density = strip_of(pq.at[0], zq.at[0, 0], zq.at[1, 0])
        source = strip_of(src, zsrc.at[0], zsrc.at[1])

        for i in range(8):
            x = i + PX
            widen_tile(x, PY - depth)
            widen_tile(x, PY + depth)
            if depth > 1:
                continue
            centre = 1.0 / density(x, PY)
            scale, weights = scaled(
                centre,
                [
                    1.0 / density(x - 1, PY),
                    1.0 / density(x + 1, PY),
                    1.0 / density(x, PY - 1),
                    1.0 / density(x, PY + 1),
                    pltpu.roll(centre, 1, 1),
                    pltpu.roll(centre, 127, 1),
                ],
            )
            sb[i] = source(x, PY) * scale
            for n in range(6):
                wb[n, i] = weights[n]

    def stencil(i, d):
        x = i + PX
        if d == 0:
            return [[pq[k, x + o, ROWS, :] for k in range(5)] for o in range(-2, 3)]
        if d == 1:
            return [[pq[k, x, pl.ds(PY + o, 8), :] for k in range(5)] for o in range(-2, 3)]
        here = [pq[k, x, ROWS, :] for k in range(5)]
        lo = [zq[0, k, x, ROWS, :] for k in range(5)]
        hi = [zq[1, k, x, ROWS, :] for k in range(5)]
        out = [[from_below(here[k], lo[k], o) for k in range(5)] for o in (2, 1)]
        out.append(here)
        out += [[from_above(here[k], hi[k], o) for k in range(5)] for o in (1, 2)]
        return out

    def base_flux(d):
        def body(i, carry):
            q = stencil(i, d)
            low, low_speed = face_state(q[0], q[1], q[2], q[3], d)
            high, high_speed = face_state(q[1], q[2], q[3], q[4], d)
            for k in range(5):
                start = pq[k, i + PX, ROWS, :] if d == 2 else base[k, i]
                base[k, i] = start - STEP_DT * (high[k] - low[k])
            for n, v in enumerate(low_speed + high_speed):
                spd[4 * d + n, i] = v * (0.5 * STEP_DT)
            return carry

        lax.fori_loop(0, 8, body, 0)

    sources = (src, zsrc.at[0], zsrc.at[1])
    far_lines = [o for o in BESIDE if o[0]]
    near_lines = [o for o in BESIDE if not o[0]]
    for planes, lines, faces in (((0, 7, 1, 6), far_lines, FACES[2:4]), ((2, 5, 3, 4), near_lines, FACES[:2] + FACES[4:])):
        for i in planes:
            prepare(i)
        for i in planes:
            relax(0, i + PX, PY)
        if lines is far_lines:
            for o in DIAGONAL:
                share(SIGMA_1, o, *sigma(1), 0, 1)
        pack_lines(1, lines, sg.at[1], 1)
        share_lines(SIGMA_1, 1, lines, 1)
        for o in faces:
            share(SOURCE, o, *sources, 0, 1)
            share(SIGMA_1, o, *sigma(1), 0, 2)
    for o in FACES[:4]:
        share(LATE, o, *sources, 1, 2)
        share(LATE, o, *fields(0, 1), 2, 3)
    for o in DIAGONAL:
        share(LATE, o, *fields(0, 1), 1, 2, 0, 1)
        share(LATE, o, *fields(0, 1), 0, 1, 1, 2)
    for o in FACES[:4]:
        share(SECOND, o, *fields(1, 3), 1, 2)
        share(SECOND, o, *fields(4, 1), 0, 2)

    arrived(ENERGY)
    base_flux(2)
    arrived(DENSITY, SOURCE)
    spread_lines(0, zq.at[0, 0], zq.at[1, 0], 2)
    widen(1)
    arrived(SIGMA_1)
    spread_lines(1, zs.at[1, 0], zs.at[1, 1], 1)
    relax_wide(1, 1)
    for i in (0, 7, 1, 6, 2, 5):
        relax(2, i + PX, PY)
    for o in DIAGONAL:
        share(SIGMA_3, o, *sigma(3), 0, 2)
    pack_lines(2, far_lines, sg.at[3], 2)
    share_lines(SIGMA_3, 2, far_lines, 2)
    for o in FACES[2:4]:
        share(SIGMA_3, o, *sigma(3), 0, 3)
    for i in (3, 4):
        relax(2, i + PX, PY)
    pack_lines(2, near_lines, sg.at[3], 2)
    share_lines(SIGMA_3, 2, near_lines, 2)
    for o in FACES[:2] + FACES[4:]:
        share(SIGMA_3, o, *sigma(3), 0, 3)
    arrived(LATE)
    widen(2)
    arrived(SECOND)
    base_flux(0)
    base_flux(1)
    arrived(SIGMA_3)
    spread_lines(2, zs.at[3, 0], zs.at[3, 1], 2)
    relax_wide(3, 2)

    for i in range(8):
        x = i + PX
        here = sg[SWEEPS, x, ROWS, :]
        sig[i] = here
        lo, hi = zs[SWEEPS, 0, x, ROWS, :], zs[SWEEPS, 1, x, ROWS, :]
        lines = [
            [sg[SWEEPS, x + o, ROWS, :] for o in range(-2, 3)],
            [sg[SWEEPS, x, pl.ds(PY + o, 8), :] for o in range(-2, 3)],
            [from_below(here, lo, 2), from_below(here, lo, 1), here, from_above(here, hi, 1), from_above(here, hi, 2)],
        ]
        adv[0, i] = base[0, i]
        total = base[4, i]
        for d in range(3):
            v = lines[d]
            left = [(5.0 / 6.0) * v[1 + e] + (1.0 / 3.0) * v[2 + e] - (1.0 / 6.0) * v[e] for e in range(2)]
            right = [(1.0 / 3.0) * v[1 + e] + (5.0 / 6.0) * v[2 + e] - (1.0 / 6.0) * v[3 + e] for e in range(2)]
            adv[1 + d, i] = base[1 + d, i] - (0.5 * STEP_DT) * ((left[1] + right[1]) - (left[0] + right[0]))
            total = total - (
                (left[1] * spd[4 * d + 2, i] + right[1] * spd[4 * d + 3, i])
                - (left[0] * spd[4 * d, i] + right[0] * spd[4 * d + 1, i])
            )
        adv[4, i] = total

    all_rows(sum(sent), FIRST).wait_send()


def write_out(adv, sig, adv_out, sig_out, sem):
    a = pltpu.make_async_copy(adv, adv_out, sem.at[0])
    b = pltpu.make_async_copy(sig, sig_out, sem.at[1])
    a.start()
    b.start()
    a.wait()
    b.wait()


def solution(mesh):
    sizes = {a: mesh.shape[a] for a in ("gx", "gy", "gz")}

    def on_device(conserved, sigma_guess):
        f32 = jnp.float32
        anywhere = pl.BlockSpec(memory_space=pl.ANY)
        vmem = pl.BlockSpec(memory_space=pltpu.VMEM)
        shapes = (
            jax.ShapeDtypeStruct((5, 8, 8, 128), f32),
            jax.ShapeDtypeStruct((8, 8, 128), f32),
        )
        made = pl.pallas_call(
            functools.partial(kernel, sizes),
            out_shape=shapes,
            in_specs=[anywhere, anywhere],
            out_specs=(vmem, vmem),
            scratch_shapes=[
                pltpu.VMEM((5, N_X, N_Y, 128), f32),
                pltpu.VMEM((2, 5, N_X, N_Y, 128), f32),
                pltpu.VMEM((SWEEPS + 1, N_X, N_Y, 128), f32),
                pltpu.VMEM((SWEEPS + 1, 2, N_X, N_Y, 128), f32),
                pltpu.VMEM((N_X, N_Y, 128), f32),
                pltpu.VMEM((2, N_X, N_Y, 128), f32),
                pltpu.VMEM((6, N_X, N_Y, 128), f32),
                pltpu.VMEM((N_X, N_Y, 128), f32),
                pltpu.VMEM((6, 8, 8, 128), f32),
                pltpu.VMEM((8, 8, 128), f32),
                pltpu.VMEM((5, 8, 8, 128), f32),
                pltpu.VMEM((12, 8, 8, 128), f32),
                pltpu.VMEM((4096, 128), f32),
                pltpu.VMEM((3, 8, 8, 128), f32),
                pltpu.VMEM((3, 8, 8, 128), f32),
                pltpu.SemaphoreType.DMA((2,)),
                pltpu.SemaphoreType.DMA((1,)),
                pltpu.SemaphoreType.DMA((N_GROUPS,)),
            ],
            compiler_params=pltpu.CompilerParams(collective_id=0, has_side_effects=True, vmem_limit_bytes=16777216),
        )(*[pltpu.with_memory_space_constraint(v, pltpu.HBM) for v in (conserved, sigma_guess)])
        return pl.pallas_call(
            write_out,
            out_shape=shapes,
            in_specs=[vmem, vmem],
            out_specs=(anywhere, anywhere),
            scratch_shapes=[pltpu.SemaphoreType.DMA((2,))],
            compiler_params=pltpu.CompilerParams(vmem_limit_bytes=16777216),
        )(*made)

    return jax.shard_map(
        on_device,
        mesh=mesh,
        in_specs=(P(None, "gx", "gy", "gz"), P("gx", "gy", "gz")),
        out_specs=(P(None, "gx", "gy", "gz"), P("gx", "gy", "gz")),
        check_vma=False,
    )
```

```python
import functools

import jax
import jax.numpy as jnp
from jax import lax
from jax.experimental import pallas as pl
from jax.experimental.pallas import tpu as pltpu
from jax.sharding import PartitionSpec as P

MESH = pl.DeviceIdType.MESH
SWEEPS = 4
ALPHA = 10.0
GAMMA = 1.4
LAMBDA = 3.0
STEP_DT = 0.4

PX, PY = 3, 8
N_X, N_Y = 14, 24
ROWS = pl.ds(PY, 8)
PLANES = pl.ds(PX, 8)
FACES = [(0, 1, 0), (0, -1, 0), (1, 0, 0), (-1, 0, 0), (0, 0, 1), (0, 0, -1)]
EDGES = [(i, j, k) for i in (1, -1, 0) for j in (1, -1, 0) for k in (1, -1, 0) if abs(i) + abs(j) + abs(k) == 2]
BESIDE = [o for o in EDGES if o[2]]
DIAGONAL = [o for o in EDGES if not o[2]]
FIRST, DENSITY, ENERGY, SOURCE, SIGMA_1, LATE, SECOND, SIGMA_3 = range(8)
N_GROUPS = 8


def face_state(z, a, b, c, d):
    left = [(5.0 / 6.0) * a[k] + (1.0 / 3.0) * b[k] - (1.0 / 6.0) * z[k] for k in range(5)]
    right = [(1.0 / 3.0) * a[k] + (5.0 / 6.0) * b[k] - (1.0 / 6.0) * c[k] for k in range(5)]
    rows = [None] * 5
    speeds = []
    for side, s in enumerate((left, right)):
        inv = 1.0 / s[0]
        speed = s[1 + d] * inv
        speeds.append(speed)
        kinetic = 0.5 * (s[1] * s[1] + s[2] * s[2] + s[3] * s[3]) * inv
        pressure = (GAMMA - 1.0) * (s[4] - kinetic)
        sign = 0.5 * LAMBDA if side == 0 else -0.5 * LAMBDA
        terms = [s[1 + d]]
        for k in range(3):
            t = s[1 + k] * speed
            terms.append(t + pressure if k == d else t)
        terms.append((s[4] + pressure) * speed)
        for k in range(5):
            t = 0.5 * terms[k] + sign * s[k]
            rows[k] = t if rows[k] is None else rows[k] + t
    return rows, speeds


def kernel(
    sizes, q_hbm, g_hbm, adv, sig, pq, zq, sg, zs, src, zsrc, wt, sw, wb, sb, base, spd, rows_ref, pk, rk, lsem, ssem, rsem
):
    def peer(offset):
        out = {}
        for axis, step in zip(("gx", "gy", "gz"), offset):
            if step:
                n = sizes[axis]
                out[axis] = lax.rem(lax.axis_index(axis) + (step + n), n)
        return out

    load_q = pltpu.make_async_copy(q_hbm, pq.at[:, PLANES, ROWS, :], lsem.at[0])
    load_g = pltpu.make_async_copy(g_hbm, sg.at[0, PLANES, ROWS, :], lsem.at[1])
    load_q.start()
    load_g.start()
    barrier = pltpu.get_barrier_semaphore()
    for offset in FACES:
        pl.semaphore_signal(barrier, inc=1, device_id=peer(offset), device_id_type=MESH)
    pl.semaphore_wait(barrier, 6)
    load_q.wait()
    load_g.wait()

    sent = [0] * N_GROUPS

    def send(source, target, offset, group):
        rows = 1
        for n in source.shape[:-1]:
            rows *= n
        sent[group] += rows
        pltpu.make_async_remote_copy(
            src_ref=source,
            dst_ref=target,
            send_sem=ssem.at[0],
            recv_sem=rsem.at[group],
            device_id=peer(offset),
            device_id_type=MESH,
        ).start()

    def all_rows(rows, group):
        span_ref = rows_ref.at[pl.ds(0, rows)]
        return pltpu.make_async_remote_copy(
            src_ref=span_ref,
            dst_ref=span_ref,
            send_sem=ssem.at[0],
            recv_sem=rsem.at[group],
            device_id=peer(FACES[0]),
            device_id_type=MESH,
        )

    def arrived(*groups):
        for group in groups:
            all_rows(sent[group], group).wait_recv()

    def span(step, start, near, far):
        w = far - near
        if step == 0:
            return pl.ds(start, 8), pl.ds(start, 8)
        if step > 0:
            return pl.ds(start + 8 - far, w), pl.ds(start - far, w)
        return pl.ds(start + near, w), pl.ds(start + 8 + near, w)

    def share(group, offset, centre, lower, upper, near, far, near_y=None, far_y=None):
        planes, planes_to = span(offset[0], PX, near, far)
        rows, rows_to = span(offset[1], PY, near if near_y is None else near_y, far if far_y is None else far_y)
        lead = (slice(None),) * (len(centre.shape) - 3)
        target = {0: centre, 1: lower, -1: upper}[offset[2]]
        send(
            centre.at[lead + (planes, rows, slice(None))],
            target.at[lead + (planes_to, rows_to, slice(None))],
            offset,
            group,
        )

    narrow = lax.broadcasted_iota(jnp.int32, (1, 128), 1)

    def place(start, step, layer, there):
        if there:
            return start - 1 - layer if step > 0 else start + 8 + layer
        return start + 7 - layer if step > 0 else start + layer

    def spot(offset, layer, i, there):
        if offset[0]:
            return place(PX, offset[0], layer, there), pl.ds(PY + i, 1)
        return PX + i, pl.ds(place(PY, offset[1], layer, there), 1)

    def turn(row, n):
        return pltpu.roll(row, n % 128, 1) if n % 128 else row

    def pack_lines(k, offsets, centre, depth):
        for offset in offsets:
            e = BESIDE.index(offset)
            for layer in range(depth):
                row = None
                for i in range(8):
                    x, r = spot(offset, layer, i, False)
                    v = turn(centre[x, r, :], 16 * i + (16 if offset[2] > 0 else 0))
                    row = v if row is None else jnp.where(narrow >= 16 * i, v, row)
                pk[k, e, pl.ds(layer, 1), :] = row

    def share_lines(group, k, offsets, depth):
        for offset in offsets:
            e = BESIDE.index(offset)
            send(pk.at[k, e, pl.ds(0, depth), :], rk.at[k, e, pl.ds(0, depth), :], offset, group)

    def spread_lines(k, lower, upper, depth):
        for e, offset in enumerate(BESIDE):
            target = lower if offset[2] > 0 else upper
            for layer in range(depth):
                row = rk[k, e, pl.ds(layer, 1), :]
                for i in range(8):
                    x, r = spot(offset, layer, i, True)
                    target[x, r, :] = turn(row, -16 * i - (16 if offset[2] > 0 else 0))

    def sigma(s):
        return sg.at[s], zs.at[s, 0], zs.at[s, 1]

    def fields(a, n):
        k = pl.ds(a, n)
        return pq.at[k], zq.at[0, k], zq.at[1, k]

    for o in FACES:
        share(FIRST, o, *fields(0, 4), 0, 1)
        share(FIRST, o, *sigma(0), 0, 1)

    lane = lax.broadcasted_iota(jnp.int32, (8, 128), 1)

    def from_below(x, lower, n):
        return pltpu.roll(jnp.where(lane >= 128 - n, lower, x), n, 1)

    def from_above(x, upper, n):
        return pltpu.roll(jnp.where(lane < n, upper, x), 128 - n, 1)

    def strip(lower, here, upper):
        outer = jnp.where(lane >= 64, lower, here)
        inner = jnp.where(lane >= 64, here, upper)
        return jnp.where((lane >= 32) & (lane < 96), pltpu.roll(inner, 64, 1), outer)

    pack_lines(0, BESIDE, pq.at[0], 2)
    arrived(FIRST)
    for o in DIAGONAL:
        share(DENSITY, o, *fields(0, 1), 0, 1)
    share_lines(DENSITY, 0, BESIDE, 2)
    for o in FACES[:4]:
        share(DENSITY, o, *fields(0, 1), 1, 2)
    for o in FACES[4:]:
        share(ENERGY, o, *fields(4, 1), 0, 2)

    def scaled(centre, around):
        weights = [0.5 * (centre + n) for n in around]
        total = weights[0]
        for w in weights[1:]:
            total = total + w
        scale = ALPHA / (centre + ALPHA * total)
        return scale, [w * scale for w in weights]

    def prepare(i):
        x = i + PX

        def primitive(plane, row):
            inv = 1.0 / pq[0, plane, pl.ds(row, 8), :]
            return [inv] + [pq[1 + k, plane, pl.ds(row, 8), :] * inv for k in range(3)]

        def beyond(side):
            inv = 1.0 / zq[side, 0, x, ROWS, :]
            return [inv] + [zq[side, 1 + k, x, ROWS, :] * inv for k in range(3)]

        centre = primitive(x, PY)
        lo, hi = beyond(0), beyond(1)
        pairs = [
            (primitive(x - 1, PY), primitive(x + 1, PY)),
            (primitive(x, PY - 1), primitive(x, PY + 1)),
            ([from_below(centre[k], lo[k], 1) for k in range(4)], [from_above(centre[k], hi[k], 1) for k in range(4)]),
        ]
        grad = [[0.5 * (pairs[j][1][1 + k] - pairs[j][0][1 + k]) for j in range(3)] for k in range(3)]
        div = grad[0][0] + grad[1][1] + grad[2][2]
        source = div * div
        for k in range(3):
            source = source + grad[k][k] * grad[k][k]
        source = source + 2.0 * (grad[0][1] * grad[1][0] + grad[0][2] * grad[2][0] + grad[1][2] * grad[2][1])
        scale, weights = scaled(centre[0], [pairs[j][e][0] for j in range(3) for e in range(2)])
        src[x, ROWS, :] = source
        sw[x, ROWS, :] = source * scale
        for n in range(6):
            wt[n, x, ROWS, :] = weights[n]

    def relax(s, x, row):
        r = pl.ds(row, 8)
        here = sg[s, x, r, :]
        near = [
            sg[s, x - 1, r, :],
            sg[s, x + 1, r, :],
            sg[s, x, pl.ds(row - 1, 8), :],
            sg[s, x, pl.ds(row + 1, 8), :],
            from_below(here, zs[s, 0, x, r, :], 1),
            from_above(here, zs[s, 1, x, r, :], 1),
        ]
        value = sw[x, r, :]
        for n in range(6):
            value = value + wt[n, x, r, :] * near[n]
        sg[s + 1, x, r, :] = value

    def strip_of(centre, lower, upper):
        return lambda x, row: strip(*[v[x, pl.ds(row, 8), :] for v in (lower, centre, upper)])

    def relax_strips(s):
        at = strip_of(*sigma(s))
        level = [at(x, PY) for x in range(PX - 1, PX + 9)]
        for i in range(8):
            x = i + PX
            here = level[i + 1]
            near = [
                level[i],
                level[i + 2],
                at(x, PY - 1),
                at(x, PY + 1),
                pltpu.roll(here, 1, 1),
                pltpu.roll(here, 127, 1),
            ]
            value = sb[i]
            for n in range(6):
                value = value + wb[n, i] * near[n]
            zs[s + 1, 0, x, ROWS, :] = value
            zs[s + 1, 1, x, ROWS, :] = pltpu.roll(value, 64, 1)

    def relax_wide(s, depth):
        for x in [*range(PX - depth, PX), *range(PX + 8, PX + 8 + depth)]:
            relax(s, x, PY)
        for x in range(PX, PX + 8):
            relax(s, x, PY - depth)
            relax(s, x, PY + depth)
        relax_strips(s)

    def widen_tile(x, row):
        r = pl.ds(row, 8)
        centre = 1.0 / pq[0, x, r, :]
        scale, weights = scaled(
            centre,
            [
                1.0 / pq[0, x - 1, r, :],
                1.0 / pq[0, x + 1, r, :],
                1.0 / pq[0, x, pl.ds(row - 1, 8), :],
                1.0 / pq[0, x, pl.ds(row + 1, 8), :],
                from_below(centre, 1.0 / zq[0, 0, x, r, :], 1),
                from_above(centre, 1.0 / zq[1, 0, x, r, :], 1),
            ],
        )
        sw[x, r, :] = src[x, r, :] * scale
        for n in range(6):
            wt[n, x, r, :] = weights[n]

    def widen(depth):
        for x in [*range(PX - depth, PX), *range(PX + 8, PX + 8 + depth)]:
            widen_tile(x, PY)
        density = strip_of(pq.at[0], zq.at[0, 0], zq.at[1, 0])
        source = strip_of(src, zsrc.at[0], zsrc.at[1])

        for i in range(8):
            x = i + PX
            widen_tile(x, PY - depth)
            widen_tile(x, PY + depth)
            if depth > 1:
                continue
            centre = 1.0 / density(x, PY)
            scale, weights = scaled(
                centre,
                [
                    1.0 / density(x - 1, PY),
                    1.0 / density(x + 1, PY),
                    1.0 / density(x, PY - 1),
                    1.0 / density(x, PY + 1),
                    pltpu.roll(centre, 1, 1),
                    pltpu.roll(centre, 127, 1),
                ],
            )
            sb[i] = source(x, PY) * scale
            for n in range(6):
                wb[n, i] = weights[n]

    def stencil(i, d):
        x = i + PX
        if d == 0:
            return [[pq[k, x + o, ROWS, :] for k in range(5)] for o in range(-2, 3)]
        if d == 1:
            return [[pq[k, x, pl.ds(PY + o, 8), :] for k in range(5)] for o in range(-2, 3)]
        here = [pq[k, x, ROWS, :] for k in range(5)]
        lo = [zq[0, k, x, ROWS, :] for k in range(5)]
        hi = [zq[1, k, x, ROWS, :] for k in range(5)]
        out = [[from_below(here[k], lo[k], o) for k in range(5)] for o in (2, 1)]
        out.append(here)
        out += [[from_above(here[k], hi[k], o) for k in range(5)] for o in (1, 2)]
        return out

    def base_flux(d):
        def body(i, carry):
            q = stencil(i, d)
            low, low_speed = face_state(q[0], q[1], q[2], q[3], d)
            high, high_speed = face_state(q[1], q[2], q[3], q[4], d)
            for k in range(5):
                start = pq[k, i + PX, ROWS, :] if d == 2 else base[k, i]
                base[k, i] = start - STEP_DT * (high[k] - low[k])
            for n, v in enumerate(low_speed + high_speed):
                spd[4 * d + n, i] = v * (0.5 * STEP_DT)
            return carry

        lax.fori_loop(0, 8, body, 0)

    sources = (src, zsrc.at[0], zsrc.at[1])
    far_lines = [o for o in BESIDE if o[0]]
    near_lines = [o for o in BESIDE if not o[0]]
    for planes, lines, faces in (((0, 7, 1, 6), far_lines, FACES[2:4]), ((2, 5, 3, 4), near_lines, FACES[:2] + FACES[4:])):
        for i in planes:
            prepare(i)
        for i in planes:
            relax(0, i + PX, PY)
        if lines is far_lines:
            for o in DIAGONAL:
                share(SIGMA_1, o, *sigma(1), 0, 1)
            pack_lines(1, lines, sg.at[1], 1)
            share_lines(SIGMA_1, 1, lines, 1)
        for o in faces:
            share(SOURCE, o, *sources, 0, 1)
            share(SIGMA_1, o, *sigma(1), 0, 2)
        if lines is near_lines:
            pack_lines(1, lines, sg.at[1], 1)
            share_lines(SIGMA_1, 1, lines, 1)
    for o in FACES[:4]:
        share(LATE, o, *sources, 1, 2)
        share(LATE, o, *fields(0, 1), 2, 3)
    for o in DIAGONAL:
        share(LATE, o, *fields(0, 1), 1, 2, 0, 1)
        share(LATE, o, *fields(0, 1), 0, 1, 1, 2)
    for o in FACES[:4]:
        share(SECOND, o, *fields(1, 3), 1, 2)
        share(SECOND, o, *fields(4, 1), 0, 2)

    arrived(ENERGY)
    base_flux(2)
    arrived(DENSITY, SOURCE)
    spread_lines(0, zq.at[0, 0], zq.at[1, 0], 2)
    widen(1)
    arrived(SIGMA_1)
    spread_lines(1, zs.at[1, 0], zs.at[1, 1], 1)
    relax_wide(1, 1)
    for i in (0, 7, 1, 6, 2, 5):
        relax(2, i + PX, PY)
    for o in DIAGONAL:
        share(SIGMA_3, o, *sigma(3), 0, 2)
    pack_lines(2, far_lines, sg.at[3], 2)
    share_lines(SIGMA_3, 2, far_lines, 2)
    for o in FACES[2:4]:
        share(SIGMA_3, o, *sigma(3), 0, 3)
    for i in (3, 4):
        relax(2, i + PX, PY)
    for o in FACES[:2] + FACES[4:]:
        share(SIGMA_3, o, *sigma(3), 0, 3)
    pack_lines(2, near_lines, sg.at[3], 2)
    share_lines(SIGMA_3, 2, near_lines, 2)
    arrived(LATE)
    widen(2)
    arrived(SECOND)
    base_flux(0)
    base_flux(1)
    arrived(SIGMA_3)
    spread_lines(2, zs.at[3, 0], zs.at[3, 1], 2)
    relax_wide(3, 2)

    for i in range(8):
        x = i + PX
        here = sg[SWEEPS, x, ROWS, :]
        sig[i] = here
        lo, hi = zs[SWEEPS, 0, x, ROWS, :], zs[SWEEPS, 1, x, ROWS, :]
        lines = [
            [sg[SWEEPS, x + o, ROWS, :] for o in range(-2, 3)],
            [sg[SWEEPS, x, pl.ds(PY + o, 8), :] for o in range(-2, 3)],
            [from_below(here, lo, 2), from_below(here, lo, 1), here, from_above(here, hi, 1), from_above(here, hi, 2)],
        ]
        adv[0, i] = base[0, i]
        total = base[4, i]
        for d in range(3):
            v = lines[d]
            left = [(5.0 / 6.0) * v[1 + e] + (1.0 / 3.0) * v[2 + e] - (1.0 / 6.0) * v[e] for e in range(2)]
            right = [(1.0 / 3.0) * v[1 + e] + (5.0 / 6.0) * v[2 + e] - (1.0 / 6.0) * v[3 + e] for e in range(2)]
            adv[1 + d, i] = base[1 + d, i] - (0.5 * STEP_DT) * ((left[1] + right[1]) - (left[0] + right[0]))
            total = total - (
                (left[1] * spd[4 * d + 2, i] + right[1] * spd[4 * d + 3, i])
                - (left[0] * spd[4 * d, i] + right[0] * spd[4 * d + 1, i])
            )
        adv[4, i] = total

    all_rows(sum(sent), FIRST).wait_send()


def write_out(adv, sig, adv_out, sig_out, sem):
    a = pltpu.make_async_copy(adv, adv_out, sem.at[0])
    b = pltpu.make_async_copy(sig, sig_out, sem.at[1])
    a.start()
    b.start()
    a.wait()
    b.wait()


def solution(mesh):
    sizes = {a: mesh.shape[a] for a in ("gx", "gy", "gz")}

    def on_device(conserved, sigma_guess):
        f32 = jnp.float32
        anywhere = pl.BlockSpec(memory_space=pl.ANY)
        vmem = pl.BlockSpec(memory_space=pltpu.VMEM)
        shapes = (
            jax.ShapeDtypeStruct((5, 8, 8, 128), f32),
            jax.ShapeDtypeStruct((8, 8, 128), f32),
        )
        made = pl.pallas_call(
            functools.partial(kernel, sizes),
            out_shape=shapes,
            in_specs=[anywhere, anywhere],
            out_specs=(vmem, vmem),
            scratch_shapes=[
                pltpu.VMEM((5, N_X, N_Y, 128), f32),
                pltpu.VMEM((2, 5, N_X, N_Y, 128), f32),
                pltpu.VMEM((SWEEPS + 1, N_X, N_Y, 128), f32),
                pltpu.VMEM((SWEEPS + 1, 2, N_X, N_Y, 128), f32),
                pltpu.VMEM((N_X, N_Y, 128), f32),
                pltpu.VMEM((2, N_X, N_Y, 128), f32),
                pltpu.VMEM((6, N_X, N_Y, 128), f32),
                pltpu.VMEM((N_X, N_Y, 128), f32),
                pltpu.VMEM((6, 8, 8, 128), f32),
                pltpu.VMEM((8, 8, 128), f32),
                pltpu.VMEM((5, 8, 8, 128), f32),
                pltpu.VMEM((12, 8, 8, 128), f32),
                pltpu.VMEM((4096, 128), f32),
                pltpu.VMEM((3, 8, 8, 128), f32),
                pltpu.VMEM((3, 8, 8, 128), f32),
                pltpu.SemaphoreType.DMA((2,)),
                pltpu.SemaphoreType.DMA((1,)),
                pltpu.SemaphoreType.DMA((N_GROUPS,)),
            ],
            compiler_params=pltpu.CompilerParams(collective_id=0, has_side_effects=True, vmem_limit_bytes=16777216),
        )(*[pltpu.with_memory_space_constraint(v, pltpu.HBM) for v in (conserved, sigma_guess)])
        return pl.pallas_call(
            write_out,
            out_shape=shapes,
            in_specs=[vmem, vmem],
            out_specs=(anywhere, anywhere),
            scratch_shapes=[pltpu.SemaphoreType.DMA((2,))],
            compiler_params=pltpu.CompilerParams(vmem_limit_bytes=16777216),
        )(*made)

    return jax.shard_map(
        on_device,
        mesh=mesh,
        in_specs=(P(None, "gx", "gy", "gz"), P("gx", "gy", "gz")),
        out_specs=(P(None, "gx", "gy", "gz"), P("gx", "gy", "gz")),
        check_vma=False,
    )
```
